512 devices in a mesh: cell: 32 (over x, y), gene: 16 (over z, core).
Axes of the slice: x: 4, y: 8, z: 8, core: 2. Of those that a mesh axis runs over, the one named last changes fastest.
Arguments:
- counts: int32 [8192, 10240], P('cell', 'gene'), may hold values from 1 to 8
- cell_factors: float32 [64, 8192], P(None, 'cell'), may hold values from -6 to 6
- loadings: float32 [64, 10240], P(None, 'gene'), may hold values from -3 to 3
- cell_momenta: float32 [64, 8192], P(None, 'cell'), may hold values from -6 to 6
- loading_momenta: float32 [64, 10240], P(None, 'gene'), may hold values from -6 to 6
- step: float32 [64], replicated, may hold values from 0.01 to 0.04
Outputs:
- new_factors: float32 [64, 8192], P(None, 'cell')
- new_loadings: float32 [64, 10240], P(None, 'gene')
- new_cell_momenta: float32 [64, 8192], P(None, 'cell')
- new_loading_momenta: float32 [64, 10240], P(None, 'gene')
- log_rate: bfloat16 [8192, 10240], P('cell', 'gene')
The draws below stay inside these ranges and needn't reach their ends.
All inputs are finite; a program needn't handle non-finite values.
Results may differ from the reference program's by a relative error of at most 0.001.
Values sent between devices are 32-bit elements; how exact they have to be, the bound alone decides.
A program may use at most 64 MiB of HBM per device.

```python
import math
import jax
import jax.numpy as jnp
from jax import lax

K = 64
CELL_DEV = 256
LEAPS = 1
CELLS = 8192
GENES = 10240
N_CELL = 32


def touch_ends(array, rng, least, high):
    longest = array.shape.index(max(array.shape))
    spots = []
    for shift in (0, 1):
        where = [jax.random.randint(jax.random.fold_in(rng, axis), (), 0, length) for axis, length in enumerate(array.shape)]
        where[longest] = (where[longest] + shift) % array.shape[longest]
        spots.append(tuple(where))
    return array.at[spots[0]].set(least).at[spots[1]].set(high)


def levels(stream_key, extent, shards, low, high):
    def one(dim, shards_of):
        draws = jax.random.uniform(jax.random.fold_in(jax.random.fold_in(stream_key, 6), dim), (shards_of,), jnp.float32, low / len(shards), high / len(shards))
        return jnp.repeat(jnp.exp(draws), extent[dim] // shards_of).reshape((-1,) + (1,) * (len(extent) - dim - 1))

    loudness = one(*shards[0])
    for cut in shards[1:]:
        loudness = loudness * one(*cut)
    return loudness


def gaussian(rng, extent, scale, reach, cuts=(), kind=jnp.bfloat16):
    drawn = jax.random.normal(rng, extent, jnp.float32) * scale
    if len(cuts) > 0:
        drawn = levels(rng, extent, cuts, -0.22, 0.18) * drawn
    return jnp.clip(drawn, min=-reach, max=reach).astype(kind)


def setup_inputs(seed: int = 0) -> dict:
    seeds = jax.random.split(jax.random.key(seed), 7)
    return {
        "counts": touch_ends(jax.random.randint(seeds[0], (CELLS, GENES), 1, 9), jax.random.fold_in(seeds[0], 1), 1, 8).astype(jnp.int32),
        "cell_factors": gaussian(seeds[1], (K, CELLS), 1.0, 6.0, ((1, 32),), jnp.float32),
        "loadings": gaussian(seeds[2], (K, GENES), 0.5, 3.0, ((1, 16),), jnp.float32),
        "cell_momenta": gaussian(seeds[3], (K, CELLS), 1.0, 6.0, ((1, 32),), jnp.float32),
        "loading_momenta": gaussian(seeds[4], (K, GENES), 1.0, 6.0, ((1, 16),), jnp.float32),
        "step": jnp.clip(jnp.exp(jax.random.uniform(seeds[5], (K,), jnp.float32, math.log(0.01), math.log(0.04))), 0.01, 0.04),
    }


def gradient(factors, loadings, counts_float, library):
    scale = 1.0 / jnp.sqrt(jnp.float32(K))
    squares = lax.optimization_barrier(jnp.sum(loadings * loadings, axis=1))
    ard = (jnp.float32(GENES) + 2.0) / (squares + 2.0)
    blocks_u = jnp.transpose(factors.reshape(K, N_CELL, CELL_DEV), (1, 0, 2))
    blocks_y = counts_float.reshape(N_CELL, CELL_DEV, GENES)
    blocks_l = library.reshape(N_CELL, CELL_DEV)

    def one_block(carry, items):
        block_u, block_y, block_l = items
        linear = lax.dot_general(block_u, loadings, (((0,), (0,)), ((), ())), precision=lax.Precision.HIGHEST) * scale
        expo = jnp.exp(linear)
        total = lax.optimization_barrier(jnp.sum(expo, axis=1))
        size = block_l / total
        resid = block_y - size[:, None] * expo
        grad_u = lax.dot_general(loadings, resid, (((1,), (1,)), ((), ())), precision=lax.Precision.HIGHEST) * scale
        part_v = jnp.dot(block_u, resid, precision=lax.Precision.HIGHEST) * scale
        rates = (linear + jnp.log(size)[:, None]).astype(jnp.bfloat16)
        return (carry + part_v, (grad_u, rates))
    start = jnp.zeros((K, GENES), jnp.float32)
    part_v, (grad_u, rates) = lax.scan(one_block, start, (blocks_u, blocks_y, blocks_l))
    grad_u = jnp.transpose(grad_u, (1, 0, 2)).reshape(K, CELLS) - factors
    grad_v = part_v - ard[:, None] * loadings
    return (grad_u, grad_v, rates.reshape(CELLS, GENES))

def reference(counts, cell_factors, loadings, cell_momenta, loading_momenta, step):
    counts_float = counts.astype(jnp.float32)
    library = lax.optimization_barrier(jnp.sum(counts_float, axis=1))
    half = 0.5 * step[:, None]
    full = step[:, None]
    factors, loads = (cell_factors, loadings)
    mom_u, mom_v = (cell_momenta, loading_momenta)
    grad_u, grad_v, rates = gradient(factors, loads, counts_float, library)
    for leap in range(LEAPS):
        mom_u = mom_u + half * grad_u
        mom_v = mom_v + half * grad_v
        factors = factors + full * mom_u
        loads = loads + full * mom_v
        grad_u, grad_v, rates = gradient(factors, loads, counts_float, library)
        mom_u = mom_u + half * grad_u
        mom_v = mom_v + half * grad_v
    return (factors, loads, mom_u, mom_v, rates)
```

```python
import jax
import jax.numpy as jnp
from jax import lax
from jax.experimental import pallas as pl
from jax.experimental.pallas import tpu as pltpu
from jax.sharding import PartitionSpec as P

K = 64
CELLS = 256
GENES = 640
XS = 4
YS = 8
ZS = 8
CORES = 2
LANES = 128
N_CELL = XS * YS
N_GENE = ZS * CORES
V_TILES = (K // 8) * (GENES // LANES)
U_TILES = (K // 8) * (CELLS // LANES)
EXTRA = V_TILES - N_CELL
COLS = GENES // LANES
UCOLS = CELLS // LANES
MESH = pl.DeviceIdType.MESH
F32 = jnp.float32
BF16 = jnp.bfloat16


def div(a, b):
    return lax.div(a, jnp.int32(b))


def rem(a, b):
    return lax.rem(a, jnp.int32(b))


def split(x):
    high = x.astype(BF16)
    return high, (x - high.astype(F32)).astype(BF16)


def zigzag(i, n):
    sign = 1 - 2 * rem(i, 2)
    return n // 2 + sign * div(i + 1, 2)


def tiles_sum(x):
    total = x[:, 0:LANES]
    for t in range(1, x.shape[1] // LANES):
        total = total + x[:, t * LANES : (t + 1) * LANES]
    return total


def row_of(part):
    return jnp.sum(part.T, axis=0, keepdims=True)


def col_of(row, block):
    lanes = lax.broadcasted_iota(jnp.int32, (8, LANES), 1)
    wanted = lax.broadcasted_iota(jnp.int32, (8, LANES), 0) + 8 * block
    return jnp.sum(jnp.where(lanes == wanted, jnp.broadcast_to(row, (8, LANES)), 0.0), axis=1, keepdims=True)


def kernel(
    counts_h, u_h, v_h, p_h, q_h, step_h,
    u_o, v_o, p_o, q_o, rate_o,
    cnt, u0, v0, p0, q0, stp,
    y16, lin, eh, el, part, lib, amat, cmat,
    r_tot, r_ls, r_sq, pu, r_ux, r_ua, r_mu, pv, r_vx, r_ve, r_va, r_mv, mv_keep, mu_keep,
    u1, v1, pfin, qfin, rate_v,
    in_sem, out_sem, send_sem, recv_sem, row_sem,
):
    cell = lax.axis_index("cell")
    gene = lax.axis_index("gene")
    cx, cy = div(cell, YS), rem(cell, YS)
    gz, gc = div(gene, CORES), rem(gene, CORES)
    owns_extra = rem(cy, XS) == cx

    loads = {}
    for n, (src, dst) in enumerate(((u_h, u0), (v_h, v0), (counts_h, cnt), (q_h, q0), (step_h, stp), (p_h, p0))):
        loads[n] = pltpu.make_async_copy(src, dst, in_sem.at[n])
        loads[n].start()

    def gene_peer(s):
        i = div(s, 2)
        zz = rem(gz + zigzag(i, ZS), ZS)
        cc = rem(gc + 1 - rem(s, 2), CORES)
        return zz * CORES + cc

    def cell_peer(s):
        xx = rem(cx + zigzag(rem(s, XS), XS), XS)
        yy = rem(cy + zigzag(div(s, XS), YS), YS)
        return xx * YS + yy

    barrier = pltpu.get_barrier_semaphore()

    def greet_gene(s, c):
        pl.semaphore_signal(barrier, inc=1, device_id={"gene": gene_peer(s)}, device_id_type=MESH)
        return c

    def greet_y(s, c):
        yy = rem(cy + s, YS)
        pl.semaphore_signal(barrier, inc=1, device_id={"cell": cx * YS + yy}, device_id_type=MESH)
        return c

    def greet_x(s, c):
        xx = rem(cx + s, XS)
        pl.semaphore_signal(barrier, inc=1, device_id={"cell": xx * YS + cy}, device_id_type=MESH)
        return c

    lax.fori_loop(0, N_GENE - 1, greet_gene, 0)
    lax.fori_loop(1, YS, greet_y, 0)
    lax.fori_loop(1, XS, greet_x, 0)

    def wait_bytes(ref, sem):
        pltpu.make_async_copy(ref, ref, sem).wait()

    def push(src, dst, phase, where):
        pltpu.make_async_remote_copy(
            src_ref=src, dst_ref=dst, send_sem=send_sem.at[phase], recv_sem=recv_sem.at[phase],
            device_id=where, device_id_type=MESH,
        ).start()

    def to_genes(src_of, dst, phase):
        def body(s, c):
            peer = gene_peer(s)
            push(src_of(peer), dst, phase, {"gene": peer})
            return c
        lax.fori_loop(0, N_GENE - 1, body, 0)

    def scatter_loadings(g, phase):
        def body(s, c):
            peer = cell_peer(s)
            push(pv.at[g, peer], r_vx.at[g, cell], phase, {"cell": peer})
            px, py = div(peer, YS), rem(peer, YS)

            @pl.when(rem(py, XS) == px)
            def _():
                push(pv.at[g, N_CELL + py], r_ve.at[g, cell], phase + 1, {"cell": peer})
            return c
        lax.fori_loop(0, N_CELL - 1, body, 0)

    def gather_loadings(buf, phase):
        def body(s, c):
            peer = cell_peer(s)
            push(buf.at[cell], buf.at[cell], phase, {"cell": peer})

            @pl.when(owns_extra)
            def _():
                push(buf.at[N_CELL + cy], buf.at[N_CELL + cy], phase + 1, {"cell": peer})
            return c
        lax.fori_loop(0, N_CELL - 1, body, 0)

    def scatter_sent(g, phase):
        wait_bytes(r_vx.at[g, pl.ds(0, N_CELL - 1)], send_sem.at[phase])

        @pl.when(owns_extra)
        def _():
            wait_bytes(r_vx.at[g, pl.ds(0, EXTRA - 1)], send_sem.at[phase + 1])

        @pl.when(jnp.logical_not(owns_extra))
        def _():
            wait_bytes(r_vx.at[g, pl.ds(0, EXTRA)], send_sem.at[phase + 1])

    def gather_sent(buf, phase):
        wait_bytes(buf.at[pl.ds(0, N_CELL - 1)], send_sem.at[phase])

        @pl.when(owns_extra)
        def _():
            wait_bytes(buf.at[pl.ds(0, N_CELL - 1)], send_sem.at[phase + 1])

    def gather_arrived(buf, phase):
        wait_bytes(buf.at[pl.ds(0, N_CELL - 1)], recv_sem.at[phase])

        @pl.when(owns_extra)
        def _():
            wait_bytes(buf.at[pl.ds(0, EXTRA - 1)], recv_sem.at[phase + 1])

        @pl.when(jnp.logical_not(owns_extra))
        def _():
            wait_bytes(buf.at[pl.ds(0, EXTRA)], recv_sem.at[phase + 1])

    chunks = []
    at = 0
    while at < GENES:
        chunks.append((at, min(256, GENES - at)))
        at += 256

    def exponentials(u, v):
        uh, ul = split(u * 0.125)
        uh32, ul32 = uh.astype(F32), ul.astype(F32)
        left = jnp.concatenate([uh32, uh32, ul32, ul32], axis=0).T.astype(BF16)
        vh, vl = split(v)
        right = jnp.concatenate([vh, vl, vh, vl], axis=0)
        for n, (lo, wide) in enumerate(chunks):
            x = jnp.dot(left, right[:, lo : lo + wide], preferred_element_type=F32)
            e = jnp.exp(x)
            lin[:, lo : lo + wide] = x
            high, low = split(e)
            eh[:, lo : lo + wide] = high
            el[:, lo : lo + wide] = low
            some = tiles_sum(e)
            part[...] = some if n == 0 else part[...] + some
        return row_of(part[...])

    def square_row(v):
        s = tiles_sum(v * v)
        return row_of(jnp.concatenate([s, jnp.zeros_like(s)], axis=0))

    def stacked(x):
        high, low = split(x)
        return jnp.concatenate([high, low], axis=0), high

    def across(both):
        return both[:K] + both[K:]

    over_genes = (((1,), (1,)), ((), ()))

    def counts_by_genes(v):
        pair, _ = stacked(v * 0.125)
        amat[...] = across(lax.dot_general(pair, y16[...], over_genes, preferred_element_type=F32))

    def expo_by_genes(v):
        pair, high = stacked(v * 0.125)
        both = lax.dot_general(pair, eh[...], over_genes, preferred_element_type=F32)
        rest = lax.dot_general(high, el[...], over_genes, preferred_element_type=F32)
        return across(both) + rest

    def counts_by_cells(u):
        pair, _ = stacked(u * 0.125)
        for lo, wide in chunks:
            cmat[:, lo : lo + wide] = across(jnp.dot(pair, y16[:, lo : lo + wide], preferred_element_type=F32))

    def loadings_parts(g, u, size):
        pair, high = stacked(u * (size * 0.125))
        for lo, wide in chunks:
            both = jnp.dot(pair, eh[:, lo : lo + wide], preferred_element_type=F32)
            rest = jnp.dot(high, el[:, lo : lo + wide], preferred_element_type=F32)
            piece = cmat[:, lo : lo + wide] - (across(both) + rest)
            for t in range(wide // LANES):
                for b in range(K // 8):
                    pv[g, b * COLS + lo // LANES + t] = piece[8 * b : 8 * b + 8, t * LANES : (t + 1) * LANES]

    def factor_parts(g, bmat, size):
        cross = amat[...] - size * bmat
        for b in range(K // 8):
            for t in range(UCOLS):
                pu[g, b * UCOLS + t] = cross[8 * b : 8 * b + 8, t * LANES : (t + 1) * LANES]

    def step_col(block):
        return col_of(stp[...], block)

    loads[0].wait()
    loads[1].wait()
    tot = exponentials(u0[...], v0[...])
    loads[2].wait()
    yf = cnt[...].astype(F32)
    y16[...] = yf.astype(BF16)
    part[...] = tiles_sum(yf)
    lib_own = row_of(part[...])
    r_tot[0, gene] = tot
    r_ls[gene] = jnp.concatenate([lib_own, square_row(v0[...])], axis=1)

    pl.semaphore_wait(barrier, (N_GENE - 1) + (YS - 1) + (XS - 1))

    to_genes(lambda peer: r_tot.at[0, gene], r_tot.at[0, gene], 0)
    to_genes(lambda peer: r_ls.at[gene], r_ls.at[gene], 1)

    def tell_x(s, c):
        xx = rem(cx + s, XS)
        pl.semaphore_signal(row_sem, inc=1, device_id={"cell": xx * YS + cy}, device_id_type=MESH)
        return c

    lax.fori_loop(1, XS, tell_x, 0)

    counts_by_cells(u0[...])
    counts_by_genes(v0[...])
    bmat = expo_by_genes(v0[...])
    for n in (3, 4, 5):
        loads[n].wait()

    wait_bytes(r_tot.at[0, pl.ds(0, N_GENE - 1)], recv_sem.at[0])
    wait_bytes(r_ls.at[pl.ds(0, N_GENE - 1)], recv_sem.at[1])
    both = jnp.sum(r_ls[...], axis=0)
    lib[...] = both[:, :CELLS]
    squares = both[:, CELLS:]
    size = lib[...] / jnp.sum(r_tot[0], axis=0)
    loadings_parts(0, u0[...], size)
    pl.semaphore_wait(row_sem, XS - 1)
    scatter_loadings(0, 2)
    r_vx[0, cell] = pv[0, cell]

    factor_parts(0, bmat, size)
    to_genes(lambda peer: pu.at[0, peer], r_ux.at[0, gene], 4)
    r_ux[0, gene] = pu[0, gene]

    ub, ut = div(gene, UCOLS), rem(gene, UCOLS)
    urow, ucol = pl.multiple_of(ub * 8, 8), pl.multiple_of(ut * LANES, LANES)
    ustep = step_col(ub)
    u_tile = u0[pl.ds(urow, 8), pl.ds(ucol, LANES)]
    p_tile = p0[pl.ds(urow, 8), pl.ds(ucol, LANES)]
    wait_bytes(r_ux.at[0, pl.ds(0, N_GENE - 1)], recv_sem.at[4])
    grad = jnp.sum(r_ux[0], axis=0) - u_tile
    p_tile = p_tile + 0.5 * ustep * grad
    mu_keep[...] = p_tile
    r_ua[gene] = u_tile + ustep * p_tile
    to_genes(lambda peer: r_ua.at[gene], r_ua.at[gene], 5)

    def v_tile_of(tile):
        b, t = div(tile, COLS), rem(tile, COLS)
        row, col = pl.multiple_of(b * 8, 8), pl.multiple_of(t * LANES, LANES)
        return b, (pl.ds(row, 8), pl.ds(col, LANES))

    genes_total = float(GENES * N_GENE) + 2.0

    def first_update(tile, arrived, keep):
        b, where = v_tile_of(tile)
        vs = step_col(b)
        ard = genes_total / (col_of(squares, b) + 2.0)
        v = v0[where]
        mom = q0[where] + 0.5 * vs * (jnp.sum(arrived, axis=0) - ard * v)
        mv_keep[keep] = mom
        r_va[tile] = v + vs * mom

    def arrived_parts(g, phase):
        wait_bytes(r_vx.at[g, pl.ds(0, N_CELL - 1)], recv_sem.at[phase])

        @pl.when(owns_extra)
        def _():
            r_ve[g, cell] = pv[g, N_CELL + cy]
            wait_bytes(r_ve.at[g, pl.ds(0, N_CELL - 1)], recv_sem.at[phase + 1])

    arrived_parts(0, 2)
    first_update(cell, r_vx[0], 0)

    @pl.when(owns_extra)
    def _():
        first_update(N_CELL + cy, r_ve[0], 1)

    gather_loadings(r_va, 6)

    wait_bytes(r_ua.at[pl.ds(0, N_GENE - 1)], recv_sem.at[5])
    for b in range(K // 8):
        for t in range(UCOLS):
            u1[8 * b : 8 * b + 8, t * LANES : (t + 1) * LANES] = r_ua[b * UCOLS + t]
    out_u = pltpu.make_async_copy(u1, u_o, out_sem.at[0])
    out_u.start()
    counts_by_cells(u1[...])

    gather_arrived(r_va, 6)
    for b in range(K // 8):
        for t in range(COLS):
            v1[8 * b : 8 * b + 8, t * LANES : (t + 1) * LANES] = r_va[b * COLS + t]
    out_v = pltpu.make_async_copy(v1, v_o, out_sem.at[1])
    out_v.start()

    r_tot[1, gene] = exponentials(u1[...], v1[...])
    to_genes(lambda peer: r_tot.at[1, gene], r_tot.at[1, gene], 8)
    r_sq[gene] = square_row(v1[...])
    to_genes(lambda peer: r_sq.at[gene], r_sq.at[gene], 9)
    counts_by_genes(v1[...])
    bmat = expo_by_genes(v1[...])

    wait_bytes(r_tot.at[1, pl.ds(0, N_GENE - 1)], recv_sem.at[8])
    size = lib[...] / jnp.sum(r_tot[1], axis=0)
    loadings_parts(1, u1[...], size)
    scatter_loadings(1, 10)
    r_vx[1, cell] = pv[1, cell]

    factor_parts(1, bmat, size)
    to_genes(lambda peer: pu.at[1, peer], r_ux.at[1, gene], 12)
    r_ux[1, gene] = pu[1, gene]

    shift = jnp.broadcast_to(jnp.log(size), (LANES, CELLS)).T
    for t in range(COLS):
        rate_v[:, t * LANES : (t + 1) * LANES] = (lin[:, t * LANES : (t + 1) * LANES] + shift).astype(BF16)
    out_r = pltpu.make_async_copy(rate_v, rate_o, out_sem.at[4])
    out_r.start()

    wait_bytes(r_ux.at[1, pl.ds(0, N_GENE - 1)], recv_sem.at[12])
    u_tile = u1[pl.ds(urow, 8), pl.ds(ucol, LANES)]
    grad = jnp.sum(r_ux[1], axis=0) - u_tile
    r_mu[gene] = mu_keep[...] + 0.5 * ustep * grad
    to_genes(lambda peer: r_mu.at[gene], r_mu.at[gene], 13)

    wait_bytes(r_sq.at[pl.ds(0, N_GENE - 1)], recv_sem.at[9])
    squares2 = jnp.sum(r_sq[...], axis=0)

    def second_update(tile, arrived, keep):
        b, where = v_tile_of(tile)
        vs = step_col(b)
        ard = genes_total / (col_of(squares2, b) + 2.0)
        r_mv[tile] = mv_keep[keep] + 0.5 * vs * (jnp.sum(arrived, axis=0) - ard * v1[where])

    arrived_parts(1, 10)
    second_update(cell, r_vx[1], 0)

    @pl.when(owns_extra)
    def _():
        second_update(N_CELL + cy, r_ve[1], 1)

    gather_loadings(r_mv, 14)

    wait_bytes(r_mu.at[pl.ds(0, N_GENE - 1)], recv_sem.at[13])
    for b in range(K // 8):
        for t in range(UCOLS):
            pfin[8 * b : 8 * b + 8, t * LANES : (t + 1) * LANES] = r_mu[b * UCOLS + t]
    out_p = pltpu.make_async_copy(pfin, p_o, out_sem.at[2])
    out_p.start()

    wait_bytes(r_tot.at[0, pl.ds(0, N_GENE - 1)], send_sem.at[0])
    wait_bytes(r_ls.at[pl.ds(0, N_GENE - 1)], send_sem.at[1])
    scatter_sent(0, 2)
    wait_bytes(r_ux.at[0, pl.ds(0, N_GENE - 1)], send_sem.at[4])
    wait_bytes(r_ua.at[pl.ds(0, N_GENE - 1)], send_sem.at[5])
    gather_sent(r_va, 6)
    wait_bytes(r_tot.at[1, pl.ds(0, N_GENE - 1)], send_sem.at[8])
    wait_bytes(r_sq.at[pl.ds(0, N_GENE - 1)], send_sem.at[9])
    scatter_sent(1, 10)
    wait_bytes(r_ux.at[1, pl.ds(0, N_GENE - 1)], send_sem.at[12])
    wait_bytes(r_mu.at[pl.ds(0, N_GENE - 1)], send_sem.at[13])

    gather_arrived(r_mv, 14)
    for b in range(K // 8):
        for t in range(COLS):
            qfin[8 * b : 8 * b + 8, t * LANES : (t + 1) * LANES] = r_mv[b * COLS + t]
    out_q = pltpu.make_async_copy(qfin, q_o, out_sem.at[3])
    out_q.start()
    gather_sent(r_mv, 14)
    for copy in (out_u, out_v, out_r, out_p, out_q):
        copy.wait()


def local(counts, cell_factors, loadings, cell_momenta, loading_momenta, step):
    padded = jnp.pad(step, (0, LANES - K)).reshape(1, LANES)
    vm = pltpu.VMEM
    scratch = [
        vm((CELLS, GENES), jnp.int32), vm((K, CELLS), F32), vm((K, GENES), F32), vm((K, CELLS), F32), vm((K, GENES), F32), vm((1, LANES), F32),
        vm((CELLS, GENES), BF16), vm((CELLS, GENES), F32), vm((CELLS, GENES), BF16), vm((CELLS, GENES), BF16),
        vm((CELLS, LANES), F32), vm((1, CELLS), F32), vm((K, CELLS), F32), vm((K, GENES), F32),
        vm((2, N_GENE, 1, CELLS), F32), vm((N_GENE, 1, CELLS + LANES), F32), vm((N_GENE, 1, LANES), F32),
        vm((2, U_TILES, 8, LANES), F32), vm((2, N_GENE, 8, LANES), F32), vm((U_TILES, 8, LANES), F32), vm((U_TILES, 8, LANES), F32),
        vm((2, V_TILES, 8, LANES), F32), vm((2, N_CELL, 8, LANES), F32), vm((2, N_CELL, 8, LANES), F32),
        vm((V_TILES, 8, LANES), F32), vm((V_TILES, 8, LANES), F32), vm((2, 8, LANES), F32), vm((8, LANES), F32),
        vm((K, CELLS), F32), vm((K, GENES), F32), vm((K, CELLS), F32), vm((K, GENES), F32), vm((CELLS, GENES), BF16),
        pltpu.SemaphoreType.DMA((6,)), pltpu.SemaphoreType.DMA((5,)),
        pltpu.SemaphoreType.DMA((16,)), pltpu.SemaphoreType.DMA((16,)), pltpu.SemaphoreType.REGULAR,
    ]
    return pl.pallas_call(
        kernel,
        out_shape=(
            jax.ShapeDtypeStruct((K, CELLS), F32),
            jax.ShapeDtypeStruct((K, GENES), F32),
            jax.ShapeDtypeStruct((K, CELLS), F32),
            jax.ShapeDtypeStruct((K, GENES), F32),
            jax.ShapeDtypeStruct((CELLS, GENES), BF16),
        ),
        in_specs=[pl.BlockSpec(memory_space=pl.ANY)] * 6,
        out_specs=[pl.BlockSpec(memory_space=pl.ANY)] * 5,
        scratch_shapes=scratch,
        compiler_params=pltpu.CompilerParams(collective_id=0, has_side_effects=True, vmem_limit_bytes=48 * 1024 * 1024),
    )(counts, cell_factors, loadings, cell_momenta, loading_momenta, padded)


def solution(mesh):
    placed = (
        P("cell", "gene"),
        P(None, "cell"),
        P(None, "gene"),
        P(None, "cell"),
        P(None, "gene"),
        P(),
    )
    return jax.shard_map(
        local,
        mesh=mesh,
        in_specs=placed,
        out_specs=(
            P(None, "cell"),
            P(None, "gene"),
            P(None, "cell"),
            P(None, "gene"),
            P("cell", "gene"),
        ),
        check_vma=False,
    )
```

```python
import jax
import jax.numpy as jnp
from jax import lax
from jax.experimental import pallas as pl
from jax.experimental.pallas import tpu as pltpu
from jax.sharding import PartitionSpec as P

K = 64
CELLS = 256
GENES = 640
XS = 4
YS = 8
ZS = 8
CORES = 2
LANES = 128
N_CELL = XS * YS
N_GENE = ZS * CORES
V_TILES = (K // 8) * (GENES // LANES)
U_TILES = (K // 8) * (CELLS // LANES)
EXTRA = V_TILES - N_CELL
COLS = GENES // LANES
UCOLS = CELLS // LANES
MESH = pl.DeviceIdType.MESH
F32 = jnp.float32
BF16 = jnp.bfloat16


def div(a, b):
    return lax.div(a, jnp.int32(b))


def rem(a, b):
    return lax.rem(a, jnp.int32(b))


def split(x):
    high = x.astype(BF16)
    return high, (x - high.astype(F32)).astype(BF16)


def far_first(n):
    return sorted(range(n), key=lambda d: -min(d, n - d))


def tiles_sum(x):
    total = x[:, 0:LANES]
    for t in range(1, x.shape[1] // LANES):
        total = total + x[:, t * LANES : (t + 1) * LANES]
    return total


def row_of(part):
    return jnp.sum(part.T, axis=0, keepdims=True)


def col_of(row, block):
    shape = (8, row.shape[1])
    lanes = lax.broadcasted_iota(jnp.int32, shape, 1)
    wanted = lax.broadcasted_iota(jnp.int32, shape, 0) + 8 * block
    return jnp.sum(jnp.where(lanes == wanted, jnp.broadcast_to(row, shape), 0.0), axis=1, keepdims=True)


def kernel(
    counts_h, u_h, v_h, p_h, q_h, step_h,
    u1, v1, pfin, qfin, rate_v,
    cnt, u0, v0, p0, q0, stp,
    y16, lin, eh, el, part, lib, amat, cmat,
    r_tot, r_ls, r_sq, pu, r_ux, r_ua, r_mu, pv, r_vx, r_ve, r_va, r_mv, mv_keep, mu_keep,
    in_sem, send_sem, recv_sem, row_sem,
):
    cell = lax.axis_index("cell")
    gene = lax.axis_index("gene")
    cx, cy = div(cell, YS), rem(cell, YS)
    gz, gc = div(gene, CORES), rem(gene, CORES)
    owns_extra = rem(cy + 2 * gc, XS) == cx

    xs = [rem(cx + d, XS) * YS for d in range(XS)]
    ys = [rem(cy + d, YS) for d in range(YS)]
    zs = [rem(gz + d, ZS) * CORES for d in range(ZS)]
    cs = [gc, 1 - gc]
    gene_peers = [zs[d] + cs[c] for d in far_first(ZS) for c in (1, 0) if (d, c) != (0, 0)]

    barrier = pltpu.get_barrier_semaphore()
    for peer in gene_peers:
        pl.semaphore_signal(barrier, inc=1, device_id={"gene": peer}, device_id_type=MESH)
    for d in far_first(YS)[:-1]:
        pl.semaphore_signal(barrier, inc=1, device_id={"cell": xs[0] + ys[d]}, device_id_type=MESH)
    for d in far_first(XS)[:-1]:
        pl.semaphore_signal(barrier, inc=1, device_id={"cell": xs[d] + cy}, device_id_type=MESH)

    loads = {}
    for n, (src, dst) in enumerate(((u_h, u0), (v_h, v0), (counts_h, cnt), (q_h, q0), (step_h, stp), (p_h, p0))):
        loads[n] = pltpu.make_async_copy(src, dst, in_sem.at[n])
        loads[n].start()

    def wait_bytes(ref, sem):
        pltpu.make_async_copy(ref, ref, sem).wait()

    def push(src, dst, phase, where):
        pltpu.make_async_remote_copy(
            src_ref=src, dst_ref=dst, send_sem=send_sem.at[phase], recv_sem=recv_sem.at[phase],
            device_id=where, device_id_type=MESH,
        ).start()

    def to_genes(src_of, dst, phase):
        for peer in gene_peers:
            push(src_of(peer), dst, phase, {"gene": peer})

    def scatter_loadings(g, phase):
        for dy in far_first(YS):
            def extra(dy=dy):
                owner = rem(ys[dy] + 2 * gc, XS) * YS + ys[dy]
                push(pv.at[g, N_CELL + ys[dy]], r_ve.at[g, cell], phase + 1, {"cell": owner})
            if dy == 0:
                pl.when(jnp.logical_not(owns_extra))(extra)
            else:
                extra()
            for dx in far_first(XS):
                if (dx, dy) != (0, 0):
                    peer = xs[dx] + ys[dy]
                    push(pv.at[g, peer], r_vx.at[g, cell], phase, {"cell": peer})

    def gather_loadings(buf, phase):
        def sends(also_extra):
            for dy in far_first(YS):
                for dx in far_first(XS):
                    if (dx, dy) != (0, 0):
                        peer = xs[dx] + ys[dy]
                        push(buf.at[cell], buf.at[cell], phase, {"cell": peer})
                        if also_extra:
                            push(buf.at[N_CELL + cy], buf.at[N_CELL + cy], phase + 1, {"cell": peer})

        pl.when(owns_extra)(lambda: sends(True))
        pl.when(jnp.logical_not(owns_extra))(lambda: sends(False))

    def scatter_sent(g, phase):
        wait_bytes(r_vx.at[g, pl.ds(0, N_CELL - 1)], send_sem.at[phase])

        @pl.when(owns_extra)
        def _():
            wait_bytes(r_vx.at[g, pl.ds(0, EXTRA - 1)], send_sem.at[phase + 1])

        @pl.when(jnp.logical_not(owns_extra))
        def _():
            wait_bytes(r_vx.at[g, pl.ds(0, EXTRA)], send_sem.at[phase + 1])

    def gather_sent(buf, phase):
        wait_bytes(buf.at[pl.ds(0, N_CELL - 1)], send_sem.at[phase])

        @pl.when(owns_extra)
        def _():
            wait_bytes(buf.at[pl.ds(0, N_CELL - 1)], send_sem.at[phase + 1])

    def gather_arrived(buf, phase):
        wait_bytes(buf.at[pl.ds(0, N_CELL - 1)], recv_sem.at[phase])

        @pl.when(owns_extra)
        def _():
            wait_bytes(buf.at[pl.ds(0, EXTRA - 1)], recv_sem.at[phase + 1])

        @pl.when(jnp.logical_not(owns_extra))
        def _():
            wait_bytes(buf.at[pl.ds(0, EXTRA)], recv_sem.at[phase + 1])

    chunks = []
    at = 0
    while at < GENES:
        chunks.append((at, min(256, GENES - at)))
        at += 256

    def exponentials(u, v):
        uh, ul = split(u * 0.125)
        uh32, ul32 = uh.astype(F32), ul.astype(F32)
        left = jnp.concatenate([uh32, uh32, ul32, ul32], axis=0).T.astype(BF16)
        vh, vl = split(v)
        right = jnp.concatenate([vh, vl, vh, vl], axis=0)
        for n, (lo, wide) in enumerate(chunks):
            x = jnp.dot(left, right[:, lo : lo + wide], preferred_element_type=F32)
            e = jnp.exp(x)
            lin[:, lo : lo + wide] = x
            high, low = split(e)
            eh[:, lo : lo + wide] = high
            el[:, lo : lo + wide] = low
            some = tiles_sum(e)
            part[...] = some if n == 0 else part[...] + some
        return row_of(part[...])

    def square_row(v):
        s = tiles_sum(v * v)
        return row_of(jnp.concatenate([s, jnp.zeros_like(s)], axis=0))

    def stacked(x):
        high, low = split(x)
        return jnp.concatenate([high, low], axis=0), high

    def across(both):
        return both[:K] + both[K:]

    over_genes = (((1,), (1,)), ((), ()))

    def counts_by_genes(v):
        pair, _ = stacked(v * 0.125)
        amat[...] = across(lax.dot_general(pair, y16[...], over_genes, preferred_element_type=F32))

    def expo_by_genes(v):
        pair, high = stacked(v * 0.125)
        both = lax.dot_general(pair, eh[...], over_genes, preferred_element_type=F32)
        rest = lax.dot_general(high, el[...], over_genes, preferred_element_type=F32)
        return across(both) + rest

    def counts_by_cells(u):
        pair, _ = stacked(u * 0.125)
        for lo, wide in chunks:
            cmat[:, lo : lo + wide] = across(jnp.dot(pair, y16[:, lo : lo + wide], preferred_element_type=F32))

    def loadings_parts(g, u, size):
        pair, high = stacked(u * (size * 0.125))
        for lo, wide in chunks:
            both = jnp.dot(pair, eh[:, lo : lo + wide], preferred_element_type=F32)
            rest = jnp.dot(high, el[:, lo : lo + wide], preferred_element_type=F32)
            piece = cmat[:, lo : lo + wide] - (across(both) + rest)
            for t in range(wide // LANES):
                for b in range(K // 8):
                    pv[g, b * COLS + lo // LANES + t] = piece[8 * b : 8 * b + 8, t * LANES : (t + 1) * LANES]

    def factor_parts(g, bmat, size):
        cross = amat[...] - size * bmat
        for b in range(K // 8):
            for t in range(UCOLS):
                pu[g, b * UCOLS + t] = cross[8 * b : 8 * b + 8, t * LANES : (t + 1) * LANES]

    def step_col(block):
        return col_of(stp[...], block)

    loads[0].wait()
    loads[1].wait()
    tot = exponentials(u0[...], v0[...])
    loads[2].wait()
    yf = cnt[...].astype(F32)
    y16[...] = yf.astype(BF16)
    part[...] = tiles_sum(yf)
    lib_own = row_of(part[...])
    r_ls[gene] = jnp.concatenate([tot, lib_own, square_row(v0[...])], axis=1)

    pl.semaphore_wait(barrier, (N_GENE - 1) + (YS - 1) + (XS - 1))

    to_genes(lambda peer: r_ls.at[gene], r_ls.at[gene], 0)
    for d in far_first(XS)[:-1]:
        pl.semaphore_signal(row_sem, inc=1, device_id={"cell": xs[d] + cy}, device_id_type=MESH)

    counts_by_cells(u0[...])
    counts_by_genes(v0[...])
    bmat = expo_by_genes(v0[...])
    for n in (3, 4, 5):
        loads[n].wait()

    wait_bytes(r_ls.at[pl.ds(0, N_GENE - 1)], recv_sem.at[0])
    sums = jnp.sum(r_ls[...], axis=0)
    lib[...] = sums[:, CELLS : 2 * CELLS]
    squares = sums[:, 2 * CELLS :]
    size = lib[...] / sums[:, :CELLS]
    loadings_parts(0, u0[...], size)
    pl.semaphore_wait(row_sem, XS - 1)
    scatter_loadings(0, 2)
    r_vx[0, cell] = pv[0, cell]

    factor_parts(0, bmat, size)
    to_genes(lambda peer: pu.at[0, peer], r_ux.at[0, gene], 4)
    r_ux[0, gene] = pu[0, gene]

    ub, ut = div(gene, UCOLS), rem(gene, UCOLS)
    urow, ucol = pl.multiple_of(ub * 8, 8), pl.multiple_of(ut * LANES, LANES)
    ustep = step_col(ub)
    u_tile = u0[pl.ds(urow, 8), pl.ds(ucol, LANES)]
    p_tile = p0[pl.ds(urow, 8), pl.ds(ucol, LANES)]
    def v_tile_of(tile):
        b, t = div(tile, COLS), rem(tile, COLS)
        row, col = pl.multiple_of(b * 8, 8), pl.multiple_of(t * LANES, LANES)
        return b, (pl.ds(row, 8), pl.ds(col, LANES))

    genes_total = float(GENES * N_GENE) + 2.0

    def first_update(tile, arrived, keep):
        b, where = v_tile_of(tile)
        vs = step_col(b)
        ard = genes_total / (col_of(squares, b) + 2.0)
        v = v0[where]
        mom = q0[where] + 0.5 * vs * (jnp.sum(arrived, axis=0) - ard * v)
        mv_keep[keep] = mom
        r_va[tile] = v + vs * mom

    def arrived_parts(g, phase):
        wait_bytes(r_vx.at[g, pl.ds(0, N_CELL - 1)], recv_sem.at[phase])

        @pl.when(owns_extra)
        def _():
            r_ve[g, cell] = pv[g, N_CELL + cy]
            wait_bytes(r_ve.at[g, pl.ds(0, N_CELL - 1)], recv_sem.at[phase + 1])

    arrived_parts(0, 2)
    first_update(cell, r_vx[0], 0)

    @pl.when(owns_extra)
    def _():
        first_update(N_CELL + cy, r_ve[0], 1)

    gather_loadings(r_va, 6)

    wait_bytes(r_ux.at[0, pl.ds(0, N_GENE - 1)], recv_sem.at[4])
    grad = jnp.sum(r_ux[0], axis=0) - u_tile
    p_tile = p_tile + 0.5 * ustep * grad
    mu_keep[...] = p_tile
    r_ua[gene] = u_tile + ustep * p_tile
    to_genes(lambda peer: r_ua.at[gene], r_ua.at[gene], 5)

    wait_bytes(r_ua.at[pl.ds(0, N_GENE - 1)], recv_sem.at[5])
    for b in range(K // 8):
        for t in range(UCOLS):
            u1[8 * b : 8 * b + 8, t * LANES : (t + 1) * LANES] = r_ua[b * UCOLS + t]
    counts_by_cells(u1[...])

    gather_arrived(r_va, 6)
    for b in range(K // 8):
        for t in range(COLS):
            v1[8 * b : 8 * b + 8, t * LANES : (t + 1) * LANES] = r_va[b * COLS + t]

    r_tot[gene] = exponentials(u1[...], v1[...])
    to_genes(lambda peer: r_tot.at[gene], r_tot.at[gene], 8)
    r_sq[gene] = square_row(v1[...])
    to_genes(lambda peer: r_sq.at[gene], r_sq.at[gene], 9)
    counts_by_genes(v1[...])
    bmat = expo_by_genes(v1[...])

    wait_bytes(r_tot.at[pl.ds(0, N_GENE - 1)], recv_sem.at[8])
    size = lib[...] / jnp.sum(r_tot[...], axis=0)
    loadings_parts(1, u1[...], size)
    scatter_loadings(1, 10)
    r_vx[1, cell] = pv[1, cell]

    factor_parts(1, bmat, size)
    to_genes(lambda peer: pu.at[1, peer], r_ux.at[1, gene], 12)
    r_ux[1, gene] = pu[1, gene]

    shift = jnp.broadcast_to(jnp.log(size), (LANES, CELLS)).T
    for t in range(COLS):
        rate_v[:, t * LANES : (t + 1) * LANES] = (lin[:, t * LANES : (t + 1) * LANES] + shift).astype(BF16)

    wait_bytes(r_sq.at[pl.ds(0, N_GENE - 1)], recv_sem.at[9])
    squares2 = jnp.sum(r_sq[...], axis=0)

    def second_update(tile, arrived, keep):
        b, where = v_tile_of(tile)
        vs = step_col(b)
        ard = genes_total / (col_of(squares2, b) + 2.0)
        r_mv[tile] = mv_keep[keep] + 0.5 * vs * (jnp.sum(arrived, axis=0) - ard * v1[where])

    arrived_parts(1, 10)
    second_update(cell, r_vx[1], 0)

    @pl.when(owns_extra)
    def _():
        second_update(N_CELL + cy, r_ve[1], 1)

    gather_loadings(r_mv, 14)

    wait_bytes(r_ux.at[1, pl.ds(0, N_GENE - 1)], recv_sem.at[12])
    u_tile = u1[pl.ds(urow, 8), pl.ds(ucol, LANES)]
    grad = jnp.sum(r_ux[1], axis=0) - u_tile
    r_mu[gene] = mu_keep[...] + 0.5 * ustep * grad
    to_genes(lambda peer: r_mu.at[gene], r_mu.at[gene], 13)

    wait_bytes(r_mu.at[pl.ds(0, N_GENE - 1)], recv_sem.at[13])
    for b in range(K // 8):
        for t in range(UCOLS):
            pfin[8 * b : 8 * b + 8, t * LANES : (t + 1) * LANES] = r_mu[b * UCOLS + t]

    wait_bytes(r_ls.at[pl.ds(0, N_GENE - 1)], send_sem.at[0])
    scatter_sent(0, 2)
    wait_bytes(r_ux.at[0, pl.ds(0, N_GENE - 1)], send_sem.at[4])
    wait_bytes(r_ua.at[pl.ds(0, N_GENE - 1)], send_sem.at[5])
    gather_sent(r_va, 6)
    wait_bytes(r_tot.at[pl.ds(0, N_GENE - 1)], send_sem.at[8])
    wait_bytes(r_sq.at[pl.ds(0, N_GENE - 1)], send_sem.at[9])
    scatter_sent(1, 10)
    wait_bytes(r_ux.at[1, pl.ds(0, N_GENE - 1)], send_sem.at[12])
    wait_bytes(r_mu.at[pl.ds(0, N_GENE - 1)], send_sem.at[13])

    gather_arrived(r_mv, 14)
    for b in range(K // 8):
        for t in range(COLS):
            qfin[8 * b : 8 * b + 8, t * LANES : (t + 1) * LANES] = r_mv[b * COLS + t]
    gather_sent(r_mv, 14)


def write_out(*refs):
    sem = refs[10]
    copies = [pltpu.make_async_copy(refs[n], refs[5 + n], sem.at[n]) for n in range(5)]
    for copy in copies:
        copy.start()
    for copy in copies:
        copy.wait()


def local(counts, cell_factors, loadings, cell_momenta, loading_momenta, step):
    arrays = (counts, cell_factors, loadings, cell_momenta, loading_momenta, step.reshape(1, K))
    vm = pltpu.VMEM
    scratch = [
        vm((CELLS, GENES), jnp.int32), vm((K, CELLS), F32), vm((K, GENES), F32), vm((K, CELLS), F32), vm((K, GENES), F32), vm((1, K), F32),
        vm((CELLS, GENES), BF16), vm((CELLS, GENES), F32), vm((CELLS, GENES), BF16), vm((CELLS, GENES), BF16),
        vm((CELLS, LANES), F32), vm((1, CELLS), F32), vm((K, CELLS), F32), vm((K, GENES), F32),
        vm((N_GENE, 1, CELLS), F32), vm((N_GENE, 1, 2 * CELLS + LANES), F32), vm((N_GENE, 1, LANES), F32),
        vm((2, U_TILES, 8, LANES), F32), vm((2, N_GENE, 8, LANES), F32), vm((U_TILES, 8, LANES), F32), vm((U_TILES, 8, LANES), F32),
        vm((2, V_TILES, 8, LANES), F32), vm((2, N_CELL, 8, LANES), F32), vm((2, N_CELL, 8, LANES), F32),
        vm((V_TILES, 8, LANES), F32), vm((V_TILES, 8, LANES), F32), vm((2, 8, LANES), F32), vm((8, LANES), F32),
        pltpu.SemaphoreType.DMA((6,)),
        pltpu.SemaphoreType.DMA((16,)), pltpu.SemaphoreType.DMA((16,)), pltpu.SemaphoreType.REGULAR,
    ]
    shapes = (
        jax.ShapeDtypeStruct((K, CELLS), F32),
        jax.ShapeDtypeStruct((K, GENES), F32),
        jax.ShapeDtypeStruct((K, CELLS), F32),
        jax.ShapeDtypeStruct((K, GENES), F32),
        jax.ShapeDtypeStruct((CELLS, GENES), BF16),
    )
    results = pl.pallas_call(
        kernel,
        out_shape=shapes,
        in_specs=[pl.BlockSpec(memory_space=pltpu.HBM)] * 6,
        out_specs=[pl.BlockSpec(memory_space=pltpu.VMEM)] * 5,
        scratch_shapes=scratch,
        compiler_params=pltpu.CompilerParams(collective_id=0, has_side_effects=True, vmem_limit_bytes=48 * 1024 * 1024),
    )(*(pltpu.with_memory_space_constraint(a, pltpu.HBM) for a in arrays))
    return pl.pallas_call(
        write_out,
        out_shape=shapes,
        in_specs=[pl.BlockSpec(memory_space=pltpu.VMEM)] * 5,
        out_specs=[pl.BlockSpec(memory_space=pltpu.HBM)] * 5,
        scratch_shapes=[pltpu.SemaphoreType.DMA((5,))],
        compiler_params=pltpu.CompilerParams(vmem_limit_bytes=4 * 1024 * 1024),
    )(*results)


def solution(mesh):
    placed = (
        P("cell", "gene"),
        P(None, "cell"),
        P(None, "gene"),
        P(None, "cell"),
        P(None, "gene"),
        P(),
    )
    return jax.shard_map(
        local,
        mesh=mesh,
        in_specs=placed,
        out_specs=(
            P(None, "cell"),
            P(None, "gene"),
            P(None, "cell"),
            P(None, "gene"),
            P("cell", "gene"),
        ),
        check_vma=False,
    )
```

```python
import jax
import jax.numpy as jnp
from jax import lax
from jax.experimental import pallas as pl
from jax.experimental.pallas import tpu as pltpu
from jax.sharding import PartitionSpec as P

K = 64
CELLS = 256
GENES = 640
XS = 4
YS = 8
ZS = 8
CORES = 2
LANES = 128
N_CELL = XS * YS
N_GENE = ZS * CORES
V_TILES = (K // 8) * (GENES // LANES)
U_TILES = (K // 8) * (CELLS // LANES)
HALVES = 2 * (V_TILES - N_CELL)
COLS = GENES // LANES
UCOLS = CELLS // LANES
MESH = pl.DeviceIdType.MESH
F32 = jnp.float32
BF16 = jnp.bfloat16


def div(a, b):
    return lax.div(a, jnp.int32(b))


def rem(a, b):
    return lax.rem(a, jnp.int32(b))


def split(x):
    high = x.astype(BF16)
    return high, (x - high.astype(F32)).astype(BF16)


def far_first(n):
    return sorted(range(n), key=lambda d: -min(d, n - d))


def plane_far_first():
    every = [(dx, dy) for dy in far_first(YS) for dx in far_first(XS)]
    return sorted(every, key=lambda d: -min(d[0], XS - d[0]) - min(d[1], YS - d[1]))


def tiles_sum(x):
    total = x[:, 0:LANES]
    for t in range(1, x.shape[1] // LANES):
        total = total + x[:, t * LANES : (t + 1) * LANES]
    return total


def row_of(part):
    return jnp.sum(part.T, axis=0, keepdims=True)


def col_of(row, block):
    shape = (8, row.shape[1])
    lanes = lax.broadcasted_iota(jnp.int32, shape, 1)
    wanted = lax.broadcasted_iota(jnp.int32, shape, 0) + 8 * block
    return jnp.sum(jnp.where(lanes == wanted, jnp.broadcast_to(row, shape), 0.0), axis=1, keepdims=True)


def kernel(
    counts_h, u_h, v_h, p_h, q_h, step_h,
    u1, v1, pfin, qfin, rate_v,
    cnt, u0, v0, p0, q0, stp,
    y16, lin, eh, el, part, lib, amat, cmat,
    r_tot, r_ls, r_sq, pu, r_ux, r_ua, r_mu, pv, pvx, r_vx, r_ve, r_va, r_vah, r_mv, r_mvh, mv_keep, mv_half, mu_keep,
    in_sem, send_sem, recv_sem, row_sem,
):
    cell = lax.axis_index("cell")
    gene = lax.axis_index("gene")
    cx, cy = div(cell, YS), rem(cell, YS)
    gz, gc = div(gene, CORES), rem(gene, CORES)
    owns_extra = rem(cx + cy + gc, 2) == 0
    my_half = div(rem(cx + 16 - cy - gc, XS), 2)
    extra_slot = 2 * cy + my_half

    xs = [rem(cx + d, XS) * YS for d in range(XS)]
    ys = [rem(cy + d, YS) for d in range(YS)]
    zs = [rem(gz + d, ZS) * CORES for d in range(ZS)]
    cs = [gc, 1 - gc]
    gene_peers = [zs[d] + cs[c] for d in far_first(ZS) for c in (1, 0) if (d, c) != (0, 0)]

    barrier = pltpu.get_barrier_semaphore()
    for peer in gene_peers:
        pl.semaphore_signal(barrier, inc=1, device_id={"gene": peer}, device_id_type=MESH)
    for d in far_first(YS)[:-1]:
        pl.semaphore_signal(barrier, inc=1, device_id={"cell": xs[0] + ys[d]}, device_id_type=MESH)
    for d in far_first(XS)[:-1]:
        pl.semaphore_signal(barrier, inc=1, device_id={"cell": xs[d] + cy}, device_id_type=MESH)

    loads = {}
    for n, (src, dst) in enumerate(((u_h, u0), (v_h, v0), (counts_h, cnt), (q_h, q0), (step_h, stp), (p_h, p0))):
        loads[n] = pltpu.make_async_copy(src, dst, in_sem.at[n])
        loads[n].start()

    def wait_bytes(ref, sem):
        pltpu.make_async_copy(ref, ref, sem).wait()

    def push(src, dst, phase, where):
        pltpu.make_async_remote_copy(
            src_ref=src, dst_ref=dst, send_sem=send_sem.at[phase], recv_sem=recv_sem.at[phase],
            device_id=where, device_id_type=MESH,
        ).start()

    def to_genes(src_of, dst, phase):
        for peer in gene_peers:
            push(src_of(peer), dst, phase, {"gene": peer})

    def scatter_loadings(g, phase):
        for dy in far_first(YS):
            for h in range(2):
                owner = rem(ys[dy] + 2 * h + gc, XS) * YS + ys[dy]

                def extra(dy=dy, h=h, owner=owner):
                    push(pvx.at[g, 2 * ys[dy] + h], r_ve.at[g, cell], phase + 1, {"cell": owner})

                if dy == 0:
                    pl.when(owner != cell)(extra)
                else:
                    extra()
            for dx in far_first(XS):
                if (dx, dy) != (0, 0):
                    peer = xs[dx] + ys[dy]
                    push(pv.at[g, peer], r_vx.at[g, cell], phase, {"cell": peer})

    def gather_loadings(buf, halves, phase):
        def sends(also_extra):
            for dx, dy in plane_far_first():
                if True:
                    if (dx, dy) != (0, 0):
                        peer = xs[dx] + ys[dy]
                        push(buf.at[cell], buf.at[cell], phase, {"cell": peer})
                        if also_extra:
                            push(halves.at[extra_slot], halves.at[extra_slot], phase + 1, {"cell": peer})

        pl.when(owns_extra)(lambda: sends(True))
        pl.when(jnp.logical_not(owns_extra))(lambda: sends(False))

    def scatter_sent(g, phase):
        wait_bytes(r_vx.at[g, pl.ds(0, N_CELL - 1)], send_sem.at[phase])

        @pl.when(owns_extra)
        def _():
            wait_bytes(r_ve.at[g, pl.ds(0, HALVES - 1)], send_sem.at[phase + 1])

        @pl.when(jnp.logical_not(owns_extra))
        def _():
            wait_bytes(r_ve.at[g, pl.ds(0, HALVES)], send_sem.at[phase + 1])

    def gather_sent(phase):
        wait_bytes(r_vx.at[0, pl.ds(0, N_CELL - 1)], send_sem.at[phase])

        @pl.when(owns_extra)
        def _():
            wait_bytes(r_ve.at[0, pl.ds(0, N_CELL - 1)], send_sem.at[phase + 1])

    def gather_arrived(buf, halves, phase):
        wait_bytes(buf.at[pl.ds(0, N_CELL - 1)], recv_sem.at[phase])

        @pl.when(owns_extra)
        def _():
            wait_bytes(halves.at[pl.ds(0, HALVES - 1)], recv_sem.at[phase + 1])

        @pl.when(jnp.logical_not(owns_extra))
        def _():
            wait_bytes(halves, recv_sem.at[phase + 1])

    def put_together(out, buf, halves):
        for b in range(K // 8):
            for t in range(COLS):
                n = b * COLS + t
                cols = slice(t * LANES, (t + 1) * LANES)
                if n < N_CELL:
                    out[8 * b : 8 * b + 8, cols] = buf[n]
                else:
                    out[8 * b : 8 * b + 4, cols] = halves[2 * (n - N_CELL)]
                    out[8 * b + 4 : 8 * b + 8, cols] = halves[2 * (n - N_CELL) + 1]

    def half(x):
        return jnp.where(my_half == 1, x[4:8], x[0:4])

    chunks = []
    at = 0
    while at < GENES:
        chunks.append((at, min(256, GENES - at)))
        at += 256

    def exponentials(u, v):
        uh, ul = split(u * 0.125)
        uh32, ul32 = uh.astype(F32), ul.astype(F32)
        left = jnp.concatenate([uh32, uh32, ul32, ul32], axis=0).T.astype(BF16)
        vh, vl = split(v)
        right = jnp.concatenate([vh, vl, vh, vl], axis=0)
        for n, (lo, wide) in enumerate(chunks):
            x = jnp.dot(left, right[:, lo : lo + wide], preferred_element_type=F32)
            e = jnp.exp(x)
            lin[:, lo : lo + wide] = x
            high, low = split(e)
            eh[:, lo : lo + wide] = high
            el[:, lo : lo + wide] = low
            some = tiles_sum(e)
            part[...] = some if n == 0 else part[...] + some
        return row_of(part[...])

    def square_row(v):
        s = tiles_sum(v * v)
        return row_of(jnp.concatenate([s, jnp.zeros_like(s)], axis=0))

    def stacked(x):
        high, low = split(x)
        return jnp.concatenate([high, low], axis=0), high

    def across(both):
        return both[:K] + both[K:]

    over_genes = (((1,), (1,)), ((), ()))

    def counts_by_genes(v):
        pair, _ = stacked(v * 0.125)
        amat[...] = across(lax.dot_general(pair, y16[...], over_genes, preferred_element_type=F32))

    def expo_by_genes(v):
        pair, high = stacked(v * 0.125)
        both = lax.dot_general(pair, eh[...], over_genes, preferred_element_type=F32)
        rest = lax.dot_general(high, el[...], over_genes, preferred_element_type=F32)
        return across(both) + rest

    def counts_by_cells(u):
        pair, _ = stacked(u * 0.125)
        for lo, wide in chunks:
            cmat[:, lo : lo + wide] = across(jnp.dot(pair, y16[:, lo : lo + wide], preferred_element_type=F32))

    def loadings_parts(g, u, size):
        pair, high = stacked(u * (size * 0.125))
        for lo, wide in chunks:
            both = jnp.dot(pair, eh[:, lo : lo + wide], preferred_element_type=F32)
            rest = jnp.dot(high, el[:, lo : lo + wide], preferred_element_type=F32)
            piece = cmat[:, lo : lo + wide] - (across(both) + rest)
            for t in range(wide // LANES):
                for b in range(K // 8):
                    n = b * COLS + lo // LANES + t
                    one = piece[8 * b : 8 * b + 8, t * LANES : (t + 1) * LANES]
                    if n < N_CELL:
                        pv[g, n] = one
                    else:
                        pvx[g, 2 * (n - N_CELL)] = one[0:4]
                        pvx[g, 2 * (n - N_CELL) + 1] = one[4:8]

    def factor_parts(g, bmat, size):
        cross = amat[...] - size * bmat
        for b in range(K // 8):
            for t in range(UCOLS):
                pu[g, b * UCOLS + t] = cross[8 * b : 8 * b + 8, t * LANES : (t + 1) * LANES]

    def step_col(block):
        return col_of(stp[...], block)

    loads[0].wait()
    loads[1].wait()
    tot = exponentials(u0[...], v0[...])
    loads[2].wait()
    yf = cnt[...].astype(F32)
    y16[...] = yf.astype(BF16)
    part[...] = tiles_sum(yf)
    lib_own = row_of(part[...])
    r_ls[gene] = jnp.concatenate([tot, lib_own, square_row(v0[...])], axis=1)

    pl.semaphore_wait(barrier, (N_GENE - 1) + (YS - 1) + (XS - 1))

    to_genes(lambda peer: r_ls.at[gene], r_ls.at[gene], 0)
    for d in far_first(XS)[:-1]:
        pl.semaphore_signal(row_sem, inc=1, device_id={"cell": xs[d] + cy}, device_id_type=MESH)

    counts_by_cells(u0[...])
    counts_by_genes(v0[...])
    bmat = expo_by_genes(v0[...])
    for n in (3, 4, 5):
        loads[n].wait()

    wait_bytes(r_ls.at[pl.ds(0, N_GENE - 1)], recv_sem.at[0])
    sums = jnp.sum(r_ls[...], axis=0)
    lib[...] = sums[:, CELLS : 2 * CELLS]
    squares = sums[:, 2 * CELLS :]
    size = lib[...] / sums[:, :CELLS]
    loadings_parts(0, u0[...], size)
    pl.semaphore_wait(row_sem, XS - 1)
    scatter_loadings(0, 2)
    r_vx[0, cell] = pv[0, cell]

    factor_parts(0, bmat, size)
    to_genes(lambda peer: pu.at[0, peer], r_ux.at[0, gene], 4)
    r_ux[0, gene] = pu[0, gene]

    ub, ut = div(gene, UCOLS), rem(gene, UCOLS)
    urow, ucol = pl.multiple_of(ub * 8, 8), pl.multiple_of(ut * LANES, LANES)
    ustep = step_col(ub)
    u_tile = u0[pl.ds(urow, 8), pl.ds(ucol, LANES)]
    p_tile = p0[pl.ds(urow, 8), pl.ds(ucol, LANES)]
    def v_tile_of(tile):
        b, t = div(tile, COLS), rem(tile, COLS)
        row, col = pl.multiple_of(b * 8, 8), pl.multiple_of(t * LANES, LANES)
        return b, (pl.ds(row, 8), pl.ds(col, LANES))

    genes_total = float(GENES * N_GENE) + 2.0

    def first_update(tile, arrived):
        b, where = v_tile_of(tile)
        vs = step_col(b)
        ard = genes_total / (col_of(squares, b) + 2.0)
        v = v0[where]
        mom = q0[where] + 0.5 * vs * (jnp.sum(arrived, axis=0) - ard * v)
        mv_keep[...] = mom
        r_va[tile] = v + vs * mom

    def arrived_parts(g, phase):
        wait_bytes(r_vx.at[g, pl.ds(0, N_CELL - 1)], recv_sem.at[phase])

        @pl.when(owns_extra)
        def _():
            r_ve[g, cell] = pvx[g, extra_slot]
            wait_bytes(r_ve.at[g, pl.ds(0, N_CELL - 1)], recv_sem.at[phase + 1])

    arrived_parts(0, 2)
    first_update(cell, r_vx[0])

    @pl.when(owns_extra)
    def _():
        b, where = v_tile_of(N_CELL + cy)
        vs = half(step_col(b))
        ard = half(genes_total / (col_of(squares, b) + 2.0))
        v = half(v0[where])
        mom = half(q0[where]) + 0.5 * vs * (jnp.sum(r_ve[0], axis=0) - ard * v)
        mv_half[...] = mom
        r_vah[extra_slot] = v + vs * mom

    gather_loadings(r_va, r_vah, 6)

    wait_bytes(r_ux.at[0, pl.ds(0, N_GENE - 1)], recv_sem.at[4])
    grad = jnp.sum(r_ux[0], axis=0) - u_tile
    p_tile = p_tile + 0.5 * ustep * grad
    mu_keep[...] = p_tile
    r_ua[gene] = u_tile + ustep * p_tile
    to_genes(lambda peer: r_ua.at[gene], r_ua.at[gene], 5)

    wait_bytes(r_ua.at[pl.ds(0, N_GENE - 1)], recv_sem.at[5])
    for b in range(K // 8):
        for t in range(UCOLS):
            u1[8 * b : 8 * b + 8, t * LANES : (t + 1) * LANES] = r_ua[b * UCOLS + t]
    counts_by_cells(u1[...])

    gather_arrived(r_va, r_vah, 6)
    put_together(v1, r_va, r_vah)

    r_tot[gene] = exponentials(u1[...], v1[...])
    to_genes(lambda peer: r_tot.at[gene], r_tot.at[gene], 8)
    r_sq[gene] = square_row(v1[...])
    to_genes(lambda peer: r_sq.at[gene], r_sq.at[gene], 9)
    counts_by_genes(v1[...])
    bmat = expo_by_genes(v1[...])

    wait_bytes(r_tot.at[pl.ds(0, N_GENE - 1)], recv_sem.at[8])
    size = lib[...] / jnp.sum(r_tot[...], axis=0)
    loadings_parts(1, u1[...], size)
    scatter_loadings(1, 10)
    r_vx[1, cell] = pv[1, cell]

    factor_parts(1, bmat, size)
    to_genes(lambda peer: pu.at[1, peer], r_ux.at[1, gene], 12)
    r_ux[1, gene] = pu[1, gene]

    shift = jnp.broadcast_to(jnp.log(size), (LANES, CELLS)).T
    for t in range(COLS):
        rate_v[:, t * LANES : (t + 1) * LANES] = (lin[:, t * LANES : (t + 1) * LANES] + shift).astype(BF16)

    wait_bytes(r_sq.at[pl.ds(0, N_GENE - 1)], recv_sem.at[9])
    squares2 = jnp.sum(r_sq[...], axis=0)

    def second_update(tile, arrived):
        b, where = v_tile_of(tile)
        vs = step_col(b)
        ard = genes_total / (col_of(squares2, b) + 2.0)
        r_mv[tile] = mv_keep[...] + 0.5 * vs * (jnp.sum(arrived, axis=0) - ard * v1[where])

    arrived_parts(1, 10)
    second_update(cell, r_vx[1])

    @pl.when(owns_extra)
    def _():
        b, where = v_tile_of(N_CELL + cy)
        ard = half(genes_total / (col_of(squares2, b) + 2.0))
        grad = jnp.sum(r_ve[1], axis=0) - ard * half(v1[where])
        r_mvh[extra_slot] = mv_half[...] + 0.5 * half(step_col(b)) * grad

    gather_loadings(r_mv, r_mvh, 14)

    wait_bytes(r_ux.at[1, pl.ds(0, N_GENE - 1)], recv_sem.at[12])
    u_tile = u1[pl.ds(urow, 8), pl.ds(ucol, LANES)]
    grad = jnp.sum(r_ux[1], axis=0) - u_tile
    r_mu[gene] = mu_keep[...] + 0.5 * ustep * grad
    to_genes(lambda peer: r_mu.at[gene], r_mu.at[gene], 13)

    wait_bytes(r_mu.at[pl.ds(0, N_GENE - 1)], recv_sem.at[13])
    for b in range(K // 8):
        for t in range(UCOLS):
            pfin[8 * b : 8 * b + 8, t * LANES : (t + 1) * LANES] = r_mu[b * UCOLS + t]

    wait_bytes(r_ls.at[pl.ds(0, N_GENE - 1)], send_sem.at[0])
    scatter_sent(0, 2)
    wait_bytes(r_ux.at[0, pl.ds(0, N_GENE - 1)], send_sem.at[4])
    wait_bytes(r_ua.at[pl.ds(0, N_GENE - 1)], send_sem.at[5])
    gather_sent(6)
    wait_bytes(r_tot.at[pl.ds(0, N_GENE - 1)], send_sem.at[8])
    wait_bytes(r_sq.at[pl.ds(0, N_GENE - 1)], send_sem.at[9])
    scatter_sent(1, 10)
    wait_bytes(r_ux.at[1, pl.ds(0, N_GENE - 1)], send_sem.at[12])
    wait_bytes(r_mu.at[pl.ds(0, N_GENE - 1)], send_sem.at[13])

    gather_arrived(r_mv, r_mvh, 14)
    put_together(qfin, r_mv, r_mvh)
    gather_sent(14)


def write_out(*refs):
    sem = refs[10]
    copies = [pltpu.make_async_copy(refs[n], refs[5 + n], sem.at[n]) for n in range(5)]
    for copy in copies:
        copy.start()
    for copy in copies:
        copy.wait()


def local(counts, cell_factors, loadings, cell_momenta, loading_momenta, step):
    arrays = (counts, cell_factors, loadings, cell_momenta, loading_momenta, step.reshape(1, K))
    vm = pltpu.VMEM
    scratch = [
        vm((CELLS, GENES), jnp.int32), vm((K, CELLS), F32), vm((K, GENES), F32), vm((K, CELLS), F32), vm((K, GENES), F32), vm((1, K), F32),
        vm((CELLS, GENES), BF16), vm((CELLS, GENES), F32), vm((CELLS, GENES), BF16), vm((CELLS, GENES), BF16),
        vm((CELLS, LANES), F32), vm((1, CELLS), F32), vm((K, CELLS), F32), vm((K, GENES), F32),
        vm((N_GENE, 1, CELLS), F32), vm((N_GENE, 1, 2 * CELLS + LANES), F32), vm((N_GENE, 1, LANES), F32),
        vm((2, U_TILES, 8, LANES), F32), vm((2, N_GENE, 8, LANES), F32), vm((U_TILES, 8, LANES), F32), vm((U_TILES, 8, LANES), F32),
        vm((2, N_CELL, 8, LANES), F32), vm((2, HALVES, 4, LANES), F32), vm((2, N_CELL, 8, LANES), F32), vm((2, N_CELL, 4, LANES), F32),
        vm((N_CELL, 8, LANES), F32), vm((HALVES, 4, LANES), F32), vm((N_CELL, 8, LANES), F32), vm((HALVES, 4, LANES), F32), vm((8, LANES), F32), vm((4, LANES), F32), vm((8, LANES), F32),
        pltpu.SemaphoreType.DMA((6,)),
        pltpu.SemaphoreType.DMA((16,)), pltpu.SemaphoreType.DMA((16,)), pltpu.SemaphoreType.REGULAR,
    ]
    shapes = (
        jax.ShapeDtypeStruct((K, CELLS), F32),
        jax.ShapeDtypeStruct((K, GENES), F32),
        jax.ShapeDtypeStruct((K, CELLS), F32),
        jax.ShapeDtypeStruct((K, GENES), F32),
        jax.ShapeDtypeStruct((CELLS, GENES), BF16),
    )
    results = pl.pallas_call(
        kernel,
        out_shape=shapes,
        in_specs=[pl.BlockSpec(memory_space=pltpu.HBM)] * 6,
        out_specs=[pl.BlockSpec(memory_space=pltpu.VMEM)] * 5,
        scratch_shapes=scratch,
        compiler_params=pltpu.CompilerParams(collective_id=0, has_side_effects=True, vmem_limit_bytes=48 * 1024 * 1024),
    )(*(pltpu.with_memory_space_constraint(a, pltpu.HBM) for a in arrays))
    return pl.pallas_call(
        write_out,
        out_shape=shapes,
        in_specs=[pl.BlockSpec(memory_space=pltpu.VMEM)] * 5,
        out_specs=[pl.BlockSpec(memory_space=pltpu.HBM)] * 5,
        scratch_shapes=[pltpu.SemaphoreType.DMA((5,))],
        compiler_params=pltpu.CompilerParams(vmem_limit_bytes=4 * 1024 * 1024),
    )(*results)


def solution(mesh):
    placed = (
        P("cell", "gene"),
        P(None, "cell"),
        P(None, "gene"),
        P(None, "cell"),
        P(None, "gene"),
        P(),
    )
    return jax.shard_map(
        local,
        mesh=mesh,
        in_specs=placed,
        out_specs=(
            P(None, "cell"),
            P(None, "gene"),
            P(None, "cell"),
            P(None, "gene"),
            P("cell", "gene"),
        ),
        check_vma=False,
    )
```

```python
import jax
import jax.numpy as jnp
from jax import lax
from jax.experimental import pallas as pl
from jax.experimental.pallas import tpu as pltpu
from jax.sharding import PartitionSpec as P

K = 64
CELLS = 256
GENES = 640
XS = 4
YS = 8
ZS = 8
CORES = 2
LANES = 128
N_CELL = XS * YS
N_GENE = ZS * CORES
V_TILES = (K // 8) * (GENES // LANES)
U_TILES = (K // 8) * (CELLS // LANES)
HALVES = 2 * (V_TILES - N_CELL)
COLS = GENES // LANES
UCOLS = CELLS // LANES
MESH = pl.DeviceIdType.MESH
F32 = jnp.float32
BF16 = jnp.bfloat16


def div(a, b):
    return lax.div(a, jnp.int32(b))


def rem(a, b):
    return lax.rem(a, jnp.int32(b))


def split(x):
    high = x.astype(BF16)
    return high, (x - high.astype(F32)).astype(BF16)


def far_first(n):
    return sorted(range(n), key=lambda d: -min(d, n - d))


def plane_far_first():
    every = [(dx, dy) for dy in far_first(YS) for dx in far_first(XS)]
    return sorted(every, key=lambda d: -min(d[0], XS - d[0]) - min(d[1], YS - d[1]))


def tiles_sum(x):
    total = x[:, 0:LANES]
    for t in range(1, x.shape[1] // LANES):
        total = total + x[:, t * LANES : (t + 1) * LANES]
    return total


def row_of(part):
    return jnp.sum(part.T, axis=0, keepdims=True)


def col_of(row, block):
    shape = (8, row.shape[1])
    lanes = lax.broadcasted_iota(jnp.int32, shape, 1)
    wanted = lax.broadcasted_iota(jnp.int32, shape, 0) + 8 * block
    return jnp.sum(jnp.where(lanes == wanted, jnp.broadcast_to(row, shape), 0.0), axis=1, keepdims=True)


def kernel(
    counts_h, u_h, v_h, p_h, q_h, step_h,
    u1, v1, pfin, qfin, rate_v,
    cnt, u0, v0, p0, q0, stp,
    y16, lin, expo, eh, el, part, lib, amat, cmat,
    r_tot, r_ls, r_sq, pu, r_ux, r_ua, r_mu, pv, pvx, r_vx, r_ve, r_va, r_vah, r_mv, r_mvh, mv_keep, mv_half, mu_keep,
    in_sem, send_sem, recv_sem, row_sem,
):
    cell = lax.axis_index("cell")
    gene = lax.axis_index("gene")
    cx, cy = div(cell, YS), rem(cell, YS)
    gz, gc = div(gene, CORES), rem(gene, CORES)
    owns_extra = rem(cx + cy + gc, 2) == 0
    my_half = div(rem(cx + 16 - cy - gc, XS), 2)
    extra_slot = 2 * cy + my_half

    xs = [rem(cx + d, XS) * YS for d in range(XS)]
    ys = [rem(cy + d, YS) for d in range(YS)]
    zs = [rem(gz + d, ZS) * CORES for d in range(ZS)]
    cs = [gc, 1 - gc]
    gene_peers = [zs[d] + cs[c] for d in far_first(ZS) for c in (1, 0) if (d, c) != (0, 0)]

    barrier = pltpu.get_barrier_semaphore()
    for peer in gene_peers:
        pl.semaphore_signal(barrier, inc=1, device_id={"gene": peer}, device_id_type=MESH)
    for d in far_first(YS)[:-1]:
        pl.semaphore_signal(barrier, inc=1, device_id={"cell": xs[0] + ys[d]}, device_id_type=MESH)
    for d in far_first(XS)[:-1]:
        pl.semaphore_signal(barrier, inc=1, device_id={"cell": xs[d] + cy}, device_id_type=MESH)

    loads = {}
    for n, (src, dst) in enumerate(((u_h, u0), (v_h, v0), (counts_h, cnt), (q_h, q0), (step_h, stp), (p_h, p0))):
        loads[n] = pltpu.make_async_copy(src, dst, in_sem.at[n])
        loads[n].start()

    def wait_bytes(ref, sem):
        pltpu.make_async_copy(ref, ref, sem).wait()

    def push(src, dst, phase, where):
        pltpu.make_async_remote_copy(
            src_ref=src, dst_ref=dst, send_sem=send_sem.at[phase], recv_sem=recv_sem.at[phase],
            device_id=where, device_id_type=MESH,
        ).start()

    def to_genes(src_of, dst, phase):
        for peer in gene_peers:
            push(src_of(peer), dst, phase, {"gene": peer})

    def scatter_loadings(g, phase):
        greeted = set()
        for dx, dy in plane_far_first():
            if dy not in greeted:
                greeted.add(dy)
                for h in range(2):
                    owner = rem(ys[dy] + 2 * h + gc, XS) * YS + ys[dy]

                    def extra(dy=dy, h=h, owner=owner):
                        push(pvx.at[g, 2 * ys[dy] + h], r_ve.at[g, cell], phase + 1, {"cell": owner})

                    if dy == 0:
                        pl.when(owner != cell)(extra)
                    else:
                        extra()
            if (dx, dy) != (0, 0):
                peer = xs[dx] + ys[dy]
                push(pv.at[g, peer], r_vx.at[g, cell], phase, {"cell": peer})

    def gather_loadings(buf, halves, phase):
        def sends(also_extra):
            for dx, dy in plane_far_first():
                if True:
                    if (dx, dy) != (0, 0):
                        peer = xs[dx] + ys[dy]
                        push(buf.at[cell], buf.at[cell], phase, {"cell": peer})
                        if also_extra:
                            push(halves.at[extra_slot], halves.at[extra_slot], phase + 1, {"cell": peer})

        pl.when(owns_extra)(lambda: sends(True))
        pl.when(jnp.logical_not(owns_extra))(lambda: sends(False))

    def scatter_sent(g, phase):
        wait_bytes(r_vx.at[g, pl.ds(0, N_CELL - 1)], send_sem.at[phase])

        @pl.when(owns_extra)
        def _():
            wait_bytes(r_ve.at[g, pl.ds(0, HALVES - 1)], send_sem.at[phase + 1])

        @pl.when(jnp.logical_not(owns_extra))
        def _():
            wait_bytes(r_ve.at[g, pl.ds(0, HALVES)], send_sem.at[phase + 1])

    def gather_sent(phase):
        wait_bytes(r_vx.at[0, pl.ds(0, N_CELL - 1)], send_sem.at[phase])

        @pl.when(owns_extra)
        def _():
            wait_bytes(r_ve.at[0, pl.ds(0, N_CELL - 1)], send_sem.at[phase + 1])

    def gather_arrived(buf, halves, phase):
        wait_bytes(buf.at[pl.ds(0, N_CELL - 1)], recv_sem.at[phase])

        @pl.when(owns_extra)
        def _():
            wait_bytes(halves.at[pl.ds(0, HALVES - 1)], recv_sem.at[phase + 1])

        @pl.when(jnp.logical_not(owns_extra))
        def _():
            wait_bytes(halves, recv_sem.at[phase + 1])

    def put_together(out, buf, halves):
        for b in range(K // 8):
            for t in range(COLS):
                n = b * COLS + t
                cols = slice(t * LANES, (t + 1) * LANES)
                if n < N_CELL:
                    out[8 * b : 8 * b + 8, cols] = buf[n]
                else:
                    out[8 * b : 8 * b + 4, cols] = halves[2 * (n - N_CELL)]
                    out[8 * b + 4 : 8 * b + 8, cols] = halves[2 * (n - N_CELL) + 1]

    def half(x):
        return jnp.where(my_half == 1, x[4:8], x[0:4])

    chunks = []
    at = 0
    while at < GENES:
        chunks.append((at, min(256, GENES - at)))
        at += 256

    def exponentials(u, v):
        uh, ul = split(u * 0.125)
        uh32, ul32 = uh.astype(F32), ul.astype(F32)
        left = jnp.concatenate([uh32, uh32, ul32, ul32], axis=0).T.astype(BF16)
        vh, vl = split(v)
        right = jnp.concatenate([vh, vl, vh, vl], axis=0)
        for n, (lo, wide) in enumerate(chunks):
            x = jnp.dot(left, right[:, lo : lo + wide], preferred_element_type=F32)
            e = jnp.exp(x)
            lin[:, lo : lo + wide] = x
            expo[:, lo : lo + wide] = e
            some = tiles_sum(e)
            part[...] = some if n == 0 else part[...] + some
        return row_of(part[...])

    def in_halves():
        for lo, wide in chunks:
            high, low = split(expo[:, lo : lo + wide])
            eh[:, lo : lo + wide] = high
            el[:, lo : lo + wide] = low

    def square_row(v):
        s = tiles_sum(v * v)
        return row_of(jnp.concatenate([s, jnp.zeros_like(s)], axis=0))

    def stacked(x):
        high, low = split(x)
        return jnp.concatenate([high, low], axis=0), high

    def across(both):
        return both[:K] + both[K:]

    over_genes = (((1,), (1,)), ((), ()))

    def counts_by_genes(v):
        pair, _ = stacked(v * 0.125)
        amat[...] = across(lax.dot_general(pair, y16[...], over_genes, preferred_element_type=F32))

    def expo_by_genes(v):
        pair, high = stacked(v * 0.125)
        both = lax.dot_general(pair, eh[...], over_genes, preferred_element_type=F32)
        rest = lax.dot_general(high, el[...], over_genes, preferred_element_type=F32)
        return across(both) + rest

    def counts_by_cells(u):
        pair, _ = stacked(u * 0.125)
        for lo, wide in chunks:
            cmat[:, lo : lo + wide] = across(jnp.dot(pair, y16[:, lo : lo + wide], preferred_element_type=F32))

    def loadings_parts(g, u, size):
        pair, high = stacked(u * (size * 0.125))
        for lo, wide in chunks:
            both = jnp.dot(pair, eh[:, lo : lo + wide], preferred_element_type=F32)
            rest = jnp.dot(high, el[:, lo : lo + wide], preferred_element_type=F32)
            piece = cmat[:, lo : lo + wide] - (across(both) + rest)
            for t in range(wide // LANES):
                for b in range(K // 8):
                    n = b * COLS + lo // LANES + t
                    one = piece[8 * b : 8 * b + 8, t * LANES : (t + 1) * LANES]
                    if n < N_CELL:
                        pv[g, n] = one
                    else:
                        pvx[g, 2 * (n - N_CELL)] = one[0:4]
                        pvx[g, 2 * (n - N_CELL) + 1] = one[4:8]

    def factor_parts(g, bmat, size):
        cross = amat[...] - size * bmat
        for b in range(K // 8):
            for t in range(UCOLS):
                pu[g, b * UCOLS + t] = cross[8 * b : 8 * b + 8, t * LANES : (t + 1) * LANES]

    def step_col(block):
        return col_of(stp[...], block)

    loads[0].wait()
    loads[1].wait()
    tot = exponentials(u0[...], v0[...])
    loads[2].wait()
    yf = cnt[...].astype(F32)
    y16[...] = yf.astype(BF16)
    part[...] = tiles_sum(yf)
    lib_own = row_of(part[...])
    r_ls[gene] = jnp.concatenate([tot, lib_own, square_row(v0[...])], axis=1)

    pl.semaphore_wait(barrier, (N_GENE - 1) + (YS - 1) + (XS - 1))

    to_genes(lambda peer: r_ls.at[gene], r_ls.at[gene], 0)
    for d in far_first(XS)[:-1]:
        pl.semaphore_signal(row_sem, inc=1, device_id={"cell": xs[d] + cy}, device_id_type=MESH)

    in_halves()
    counts_by_cells(u0[...])
    counts_by_genes(v0[...])
    bmat = expo_by_genes(v0[...])
    for n in (3, 4, 5):
        loads[n].wait()

    wait_bytes(r_ls.at[pl.ds(0, N_GENE - 1)], recv_sem.at[0])
    sums = jnp.sum(r_ls[...], axis=0)
    lib[...] = sums[:, CELLS : 2 * CELLS]
    squares = sums[:, 2 * CELLS :]
    size = lib[...] / sums[:, :CELLS]
    loadings_parts(0, u0[...], size)
    pl.semaphore_wait(row_sem, XS - 1)
    scatter_loadings(0, 2)
    r_vx[0, cell] = pv[0, cell]

    factor_parts(0, bmat, size)
    to_genes(lambda peer: pu.at[0, peer], r_ux.at[0, gene], 4)
    r_ux[0, gene] = pu[0, gene]

    ub, ut = div(gene, UCOLS), rem(gene, UCOLS)
    urow, ucol = pl.multiple_of(ub * 8, 8), pl.multiple_of(ut * LANES, LANES)
    ustep = step_col(ub)
    u_tile = u0[pl.ds(urow, 8), pl.ds(ucol, LANES)]
    p_tile = p0[pl.ds(urow, 8), pl.ds(ucol, LANES)]
    def v_tile_of(tile):
        b, t = div(tile, COLS), rem(tile, COLS)
        row, col = pl.multiple_of(b * 8, 8), pl.multiple_of(t * LANES, LANES)
        return b, (pl.ds(row, 8), pl.ds(col, LANES))

    genes_total = float(GENES * N_GENE) + 2.0

    def first_update(tile, arrived):
        b, where = v_tile_of(tile)
        vs = step_col(b)
        ard = genes_total / (col_of(squares, b) + 2.0)
        v = v0[where]
        mom = q0[where] + 0.5 * vs * (jnp.sum(arrived, axis=0) - ard * v)
        mv_keep[...] = mom
        r_va[tile] = v + vs * mom

    def arrived_parts(g, phase):
        wait_bytes(r_vx.at[g, pl.ds(0, N_CELL - 1)], recv_sem.at[phase])

        @pl.when(owns_extra)
        def _():
            r_ve[g, cell] = pvx[g, extra_slot]
            wait_bytes(r_ve.at[g, pl.ds(0, N_CELL - 1)], recv_sem.at[phase + 1])

    arrived_parts(0, 2)
    first_update(cell, r_vx[0])

    @pl.when(owns_extra)
    def _():
        b, where = v_tile_of(N_CELL + cy)
        vs = half(step_col(b))
        ard = half(genes_total / (col_of(squares, b) + 2.0))
        v = half(v0[where])
        mom = half(q0[where]) + 0.5 * vs * (jnp.sum(r_ve[0], axis=0) - ard * v)
        mv_half[...] = mom
        r_vah[extra_slot] = v + vs * mom

    gather_loadings(r_va, r_vah, 6)

    wait_bytes(r_ux.at[0, pl.ds(0, N_GENE - 1)], recv_sem.at[4])
    grad = jnp.sum(r_ux[0], axis=0) - u_tile
    p_tile = p_tile + 0.5 * ustep * grad
    mu_keep[...] = p_tile
    r_ua[gene] = u_tile + ustep * p_tile
    to_genes(lambda peer: r_ua.at[gene], r_ua.at[gene], 5)

    wait_bytes(r_ua.at[pl.ds(0, N_GENE - 1)], recv_sem.at[5])
    for b in range(K // 8):
        for t in range(UCOLS):
            u1[8 * b : 8 * b + 8, t * LANES : (t + 1) * LANES] = r_ua[b * UCOLS + t]
    counts_by_cells(u1[...])

    gather_arrived(r_va, r_vah, 6)
    put_together(v1, r_va, r_vah)

    r_tot[gene] = exponentials(u1[...], v1[...])
    to_genes(lambda peer: r_tot.at[gene], r_tot.at[gene], 8)
    r_sq[gene] = square_row(v1[...])
    to_genes(lambda peer: r_sq.at[gene], r_sq.at[gene], 9)
    in_halves()
    counts_by_genes(v1[...])
    bmat = expo_by_genes(v1[...])

    wait_bytes(r_tot.at[pl.ds(0, N_GENE - 1)], recv_sem.at[8])
    size = lib[...] / jnp.sum(r_tot[...], axis=0)
    loadings_parts(1, u1[...], size)
    scatter_loadings(1, 10)
    r_vx[1, cell] = pv[1, cell]

    factor_parts(1, bmat, size)
    to_genes(lambda peer: pu.at[1, peer], r_ux.at[1, gene], 12)
    r_ux[1, gene] = pu[1, gene]

    shift = jnp.broadcast_to(jnp.log(size), (LANES, CELLS)).T
    for t in range(COLS):
        rate_v[:, t * LANES : (t + 1) * LANES] = (lin[:, t * LANES : (t + 1) * LANES] + shift).astype(BF16)

    wait_bytes(r_sq.at[pl.ds(0, N_GENE - 1)], recv_sem.at[9])
    squares2 = jnp.sum(r_sq[...], axis=0)

    def second_update(tile, arrived):
        b, where = v_tile_of(tile)
        vs = step_col(b)
        ard = genes_total / (col_of(squares2, b) + 2.0)
        r_mv[tile] = mv_keep[...] + 0.5 * vs * (jnp.sum(arrived, axis=0) - ard * v1[where])

    arrived_parts(1, 10)
    second_update(cell, r_vx[1])

    @pl.when(owns_extra)
    def _():
        b, where = v_tile_of(N_CELL + cy)
        ard = half(genes_total / (col_of(squares2, b) + 2.0))
        grad = jnp.sum(r_ve[1], axis=0) - ard * half(v1[where])
        r_mvh[extra_slot] = mv_half[...] + 0.5 * half(step_col(b)) * grad

    gather_loadings(r_mv, r_mvh, 14)

    wait_bytes(r_ux.at[1, pl.ds(0, N_GENE - 1)], recv_sem.at[12])
    u_tile = u1[pl.ds(urow, 8), pl.ds(ucol, LANES)]
    grad = jnp.sum(r_ux[1], axis=0) - u_tile
    r_mu[gene] = mu_keep[...] + 0.5 * ustep * grad
    to_genes(lambda peer: r_mu.at[gene], r_mu.at[gene], 13)

    wait_bytes(r_mu.at[pl.ds(0, N_GENE - 1)], recv_sem.at[13])
    for b in range(K // 8):
        for t in range(UCOLS):
            pfin[8 * b : 8 * b + 8, t * LANES : (t + 1) * LANES] = r_mu[b * UCOLS + t]

    wait_bytes(r_ls.at[pl.ds(0, N_GENE - 1)], send_sem.at[0])
    scatter_sent(0, 2)
    wait_bytes(r_ux.at[0, pl.ds(0, N_GENE - 1)], send_sem.at[4])
    wait_bytes(r_ua.at[pl.ds(0, N_GENE - 1)], send_sem.at[5])
    gather_sent(6)
    wait_bytes(r_tot.at[pl.ds(0, N_GENE - 1)], send_sem.at[8])
    wait_bytes(r_sq.at[pl.ds(0, N_GENE - 1)], send_sem.at[9])
    scatter_sent(1, 10)
    wait_bytes(r_ux.at[1, pl.ds(0, N_GENE - 1)], send_sem.at[12])
    wait_bytes(r_mu.at[pl.ds(0, N_GENE - 1)], send_sem.at[13])

    gather_arrived(r_mv, r_mvh, 14)
    put_together(qfin, r_mv, r_mvh)
    gather_sent(14)


def write_out(*refs):
    sem = refs[10]
    copies = [pltpu.make_async_copy(refs[n], refs[5 + n], sem.at[n]) for n in range(5)]
    for copy in copies:
        copy.start()
    for copy in copies:
        copy.wait()


def local(counts, cell_factors, loadings, cell_momenta, loading_momenta, step):
    arrays = (counts, cell_factors, loadings, cell_momenta, loading_momenta, step.reshape(1, K))
    vm = pltpu.VMEM
    scratch = [
        vm((CELLS, GENES), jnp.int32), vm((K, CELLS), F32), vm((K, GENES), F32), vm((K, CELLS), F32), vm((K, GENES), F32), vm((1, K), F32),
        vm((CELLS, GENES), BF16), vm((CELLS, GENES), F32), vm((CELLS, GENES), F32), vm((CELLS, GENES), BF16), vm((CELLS, GENES), BF16),
        vm((CELLS, LANES), F32), vm((1, CELLS), F32), vm((K, CELLS), F32), vm((K, GENES), F32),
        vm((N_GENE, 1, CELLS), F32), vm((N_GENE, 1, 2 * CELLS + LANES), F32), vm((N_GENE, 1, LANES), F32),
        vm((2, U_TILES, 8, LANES), F32), vm((2, N_GENE, 8, LANES), F32), vm((U_TILES, 8, LANES), F32), vm((U_TILES, 8, LANES), F32),
        vm((2, N_CELL, 8, LANES), F32), vm((2, HALVES, 4, LANES), F32), vm((2, N_CELL, 8, LANES), F32), vm((2, N_CELL, 4, LANES), F32),
        vm((N_CELL, 8, LANES), F32), vm((HALVES, 4, LANES), F32), vm((N_CELL, 8, LANES), F32), vm((HALVES, 4, LANES), F32), vm((8, LANES), F32), vm((4, LANES), F32), vm((8, LANES), F32),
        pltpu.SemaphoreType.DMA((6,)),
        pltpu.SemaphoreType.DMA((16,)), pltpu.SemaphoreType.DMA((16,)), pltpu.SemaphoreType.REGULAR,
    ]
    shapes = (
        jax.ShapeDtypeStruct((K, CELLS), F32),
        jax.ShapeDtypeStruct((K, GENES), F32),
        jax.ShapeDtypeStruct((K, CELLS), F32),
        jax.ShapeDtypeStruct((K, GENES), F32),
        jax.ShapeDtypeStruct((CELLS, GENES), BF16),
    )
    results = pl.pallas_call(
        kernel,
        out_shape=shapes,
        in_specs=[pl.BlockSpec(memory_space=pltpu.HBM)] * 6,
        out_specs=[pl.BlockSpec(memory_space=pltpu.VMEM)] * 5,
        scratch_shapes=scratch,
        compiler_params=pltpu.CompilerParams(collective_id=0, has_side_effects=True, vmem_limit_bytes=48 * 1024 * 1024),
    )(*(pltpu.with_memory_space_constraint(a, pltpu.HBM) for a in arrays))
    return pl.pallas_call(
        write_out,
        out_shape=shapes,
        in_specs=[pl.BlockSpec(memory_space=pltpu.VMEM)] * 5,
        out_specs=[pl.BlockSpec(memory_space=pltpu.HBM)] * 5,
        scratch_shapes=[pltpu.SemaphoreType.DMA((5,))],
        compiler_params=pltpu.CompilerParams(vmem_limit_bytes=4 * 1024 * 1024),
    )(*results)


def solution(mesh):
    placed = (
        P("cell", "gene"),
        P(None, "cell"),
        P(None, "gene"),
        P(None, "cell"),
        P(None, "gene"),
        P(),
    )
    return jax.shard_map(
        local,
        mesh=mesh,
        in_specs=placed,
        out_specs=(
            P(None, "cell"),
            P(None, "gene"),
            P(None, "cell"),
            P(None, "gene"),
            P("cell", "gene"),
        ),
        check_vma=False,
    )
```
